64 devices in a mesh: dp: 4 (over x, y), sp: 16 (over z, core).
Axes of the slice: x: 2, y: 2, z: 8, core: 2. Of those that a mesh axis runs over, the one named last changes fastest.
The devices are a block of a 4x4x8 slice.
Arguments:
- signal: bfloat16 [262144, 768], P(('dp', 'sp')), parts along dimension 0
- w_first: bfloat16 [10, 1024, 2, 64, 64], P(None, 'sp')
- w_second: bfloat16 [10, 1024, 2, 64, 64], P(None, 'sp')
Outputs:
- output: bfloat16 [262144, 768], P(('dp', 'sp')), parts along dimension 0
There are 4 independent parts. The reference program is written for one: setup_inputs(seed, part) draws one part's arguments, and reference() takes and returns one part's arrays. A program takes and returns all parts, laid end to end along the dimension named above; an argument that names none is the same for every part.
All inputs are finite; a program needn't handle non-finite values.
Results may differ from the reference program's by a relative error of at most 0.02.
Values are sent between devices in bfloat16 or wider.
A program may use at most 768 MiB of HBM per device.

```python
import jax
import jax.numpy as jnp
import math
from jax import lax

SEQ_LEN = 65536
CHANNELS = 768
BLOCK_SIZE = 64

NUM_BLOCKS = SEQ_LEN // BLOCK_SIZE
STAGES = int(math.log2(NUM_BLOCKS))


def setup_inputs(seed: int = 0, part: int = 0) -> dict:
    key_signal = jax.random.fold_in(jax.random.key(seed + 1), part)
    key_first = jax.random.key(seed + 2)
    key_second = jax.random.key(seed + 3)
    w_shape = (STAGES, NUM_BLOCKS, 2, BLOCK_SIZE, BLOCK_SIZE)
    w_scale = (2 * BLOCK_SIZE) ** -0.5
    signal = jax.random.normal(key_signal, (SEQ_LEN, CHANNELS), jnp.float32)
    w_first = jax.random.normal(key_first, w_shape, jnp.float32) * w_scale
    w_second = jax.random.normal(key_second, w_shape, jnp.float32) * w_scale
    return {"signal": signal.astype(jnp.bfloat16), "w_first": w_first.astype(jnp.bfloat16), "w_second": w_second.astype(jnp.bfloat16)}


def butterfly_stage(act_blocks, weights, distance):
    grouped = act_blocks.reshape(NUM_BLOCKS // (2 * distance), 2, distance, BLOCK_SIZE, act_blocks.shape[2])
    partner = grouped[:, ::-1].reshape(act_blocks.shape)
    paired = jnp.stack([act_blocks, partner], axis=1).astype(jnp.float32)
    mixed = jnp.einsum("ltij,ltjc->lic", weights.astype(jnp.float32), paired)
    return mixed.astype(jnp.bfloat16)


def apply_map(act_blocks, weights, distances):
    for stage, distance in enumerate(distances):
        act_blocks = butterfly_stage(act_blocks, weights[stage], distance)
    return act_blocks


def reference(signal, w_first, w_second):
    col_width = min(CHANNELS, 128)
    col_groups = CHANNELS // col_width
    grouped = signal.reshape(NUM_BLOCKS, BLOCK_SIZE, col_groups, col_width).transpose(2, 0, 1, 3)
    dist_down = [2 ** (STAGES - 1 - level) for level in range(STAGES)]
    dist_up = [2 ** level for level in range(STAGES)]

    def one_group(act_blocks):
        hidden = apply_map(act_blocks, w_first, dist_down)
        hidden = jax.nn.gelu(hidden.astype(jnp.float32), approximate=False).astype(jnp.bfloat16)
        return apply_map(hidden, w_second, dist_up)

    mapped = lax.map(one_group, grouped)
    return mapped.transpose(1, 2, 0, 3).reshape(SEQ_LEN, CHANNELS)
```

```python
import functools
import math

import jax
import jax.numpy as jnp
from jax import lax
from jax.experimental import pallas as pl
from jax.experimental.pallas import tpu as pltpu
from jax.sharding import PartitionSpec as P

MESH = pl.DeviceIdType.MESH
BF16 = jnp.bfloat16
F32 = jnp.float32
CHUNK = 256
UNROLL = 8


def gelu(x):
    return 0.5 * x * (1.0 + lax.erf(x * (0.5 ** 0.5)))


def mix_stage(src, dst, weights, stage, step, act):
    pairs = src.shape[0] // 2
    unroll = min(UNROLL, pairs)

    @pl.loop(0, pairs // unroll)
    def _(it):
        for u in range(unroll):
            p = it * unroll + u
            i = (p // step) * (2 * step) + p % step
            j = i + step
            z = jnp.concatenate([src[i], src[j]], axis=0)
            w = jnp.concatenate([weights(stage, i), weights(stage, j)], axis=0)
            o = jnp.dot(w, z, preferred_element_type=F32).astype(BF16)
            if act:
                o = gelu(o.astype(F32)).astype(BF16)
            half = o.shape[0] // 2
            dst[i] = o[:half]
            dst[j] = o[half:]


def run_stages(buf, tmp, plan):
    src, dst = buf, tmp
    for weights, stage, step, act in plan:
        mix_stage(src, dst, weights, stage, step, act)
        src, dst = dst, src
    return src


def kernel(n, groups, sub, x, wa, wb, out, r1, r2, r3, tmp, ta, tb, la, lb,
           x_snd, x_rcv, o1_snd, o1_rcv, i2_snd, i2_rcv, o2_snd, o2_rcv,
           z_snd, z_rcv, g_snd, g_rcv, l_sem):
    me = lax.axis_index("sp")
    dp = lax.axis_index("dp")
    my_part = dp % sub
    base = dp - my_part
    chunks, blocks = r1.shape[0], r1.shape[1]
    per = blocks // n
    cross = int(math.log2(n))
    local = wa.shape[0] - cross
    items = cross * per // sub
    unit = min(items, per)
    units = items // unit

    def peer(t):
        side = 1 - 2 * (t % 2)
        return (me + n // 2 + side * ((t + 1) // 2) + n) % n

    barrier = pltpu.get_barrier_semaphore()

    @pl.loop(0, n - 1)
    def _(t):
        pl.semaphore_signal(barrier, inc=1, device_id={"sp": peer(t)}, device_id_type=MESH)

    for k in range(1, sub):
        pl.semaphore_signal(barrier, inc=1, device_id={"dp": base + (my_part + k) % sub}, device_id_type=MESH)
    pl.semaphore_wait(barrier, n - 1 + sub - 1)

    def cols(c):
        return pl.ds(pl.multiple_of(c * CHUNK, CHUNK), CHUNK)

    def mine(d):
        return pl.ds(d * per, per)

    def item_of(part, q):
        first = part * items + q * unit
        return first // per, first % per

    def send_weights(m, w, first_stage, t_buf):
        for q in range(units):
            s, l0 = item_of(my_part, q)

            @pl.loop(0, n - 1)
            def _(t):
                d = peer(t)
                pltpu.make_async_remote_copy(
                    src_ref=w.at[first_stage + s, pl.ds(d * per + l0, unit)],
                    dst_ref=t_buf.at[s, me, pl.ds(l0, unit)],
                    send_sem=z_snd.at[m, q], recv_sem=z_rcv.at[m, q],
                    device_id={"sp": d}, device_id_type=MESH).start()

            pltpu.make_async_copy(
                w.at[first_stage + s, pl.ds(me * per + l0, unit)],
                t_buf.at[s, me, pl.ds(l0, unit)], z_rcv.at[m, q]).start()

    def part_ref(t_buf, part, q):
        s, l0 = item_of(part, q)
        return t_buf.at[s, :, pl.ds(l0, unit)]

    def gather_copy(m, t_buf, k, q):
        mine_ref = part_ref(t_buf, my_part, q)
        return pltpu.make_async_remote_copy(
            src_ref=mine_ref, dst_ref=mine_ref,
            send_sem=g_snd.at[m, k, q], recv_sem=g_rcv.at[m, k, q],
            device_id={"dp": base + (my_part + k) % sub}, device_id_type=MESH)

    def start_gather(m, t_buf):
        for q in range(units):
            ref = part_ref(t_buf, my_part, q)
            pltpu.make_async_copy(ref, ref, z_rcv.at[m, q]).wait()
        for k in range(1, sub):
            for q in range(units):
                gather_copy(m, t_buf, k, q).start()

    def wait_gather(m, t_buf):
        for k in range(1, sub):
            for q in range(units):
                ref = part_ref(t_buf, (my_part - k + sub) % sub, q)
                pltpu.make_async_copy(ref, ref, g_rcv.at[m, k, q]).wait()

    send_weights(0, wa, 0, ta)

    @pl.loop(0, chunks)
    def _(c):
        @pl.loop(0, n - 1)
        def _(t):
            d = peer(t)
            pltpu.make_async_remote_copy(
                src_ref=x.at[mine(d), :, cols(c)], dst_ref=r1.at[c, mine(me)],
                send_sem=x_snd.at[c], recv_sem=x_rcv.at[c],
                device_id={"sp": d}, device_id_type=MESH).start()

        pltpu.make_async_copy(x.at[mine(me), :, cols(c)], r1.at[c, mine(me)], x_rcv.at[c]).start()

    send_weights(1, wb, local, tb)
    load_a = pltpu.make_async_copy(wa.at[pl.ds(cross, local)], la, l_sem.at[0])
    load_b = pltpu.make_async_copy(wb.at[pl.ds(0, local)], lb, l_sem.at[1])
    load_a.start()
    load_b.start()

    start_gather(0, ta)
    wait_gather(0, ta)

    def exchanged(t_buf):
        return lambda s, i: t_buf[s, i // per, i % per]

    def kept(l_buf):
        return lambda s, i: l_buf[s, i]

    cross_steps = [per * 2 ** s for s in range(cross)]
    local_steps = [2 ** s for s in range(local)]
    plan_t1 = [(exchanged(ta), s, step, False) for s, step in enumerate(cross_steps[::-1])]
    plan_n = [(kept(la), s, step, step == 1) for s, step in enumerate(local_steps[::-1])]
    plan_n += [(kept(lb), s, step, False) for s, step in enumerate(local_steps)]
    plan_t2 = [(exchanged(tb), s, step, False) for s, step in enumerate(cross_steps)]

    def exchange(src, dst, c, snd, rcv):
        @pl.loop(0, n - 1)
        def _(t):
            d = peer(t)
            pltpu.make_async_remote_copy(
                src_ref=src.at[c, mine(d)], dst_ref=dst.at[c, mine(me)],
                send_sem=snd.at[c], recv_sem=rcv.at[c],
                device_id={"sp": d}, device_id_type=MESH).start()

        dst[c, mine(me)] = src[c, mine(me)]

    def others(ref, c):
        return ref.at[c, pl.ds(0, (n - 1) * per)]

    def wait_for(ref, sem):
        pltpu.make_async_copy(ref, ref, sem).wait()

    @pl.loop(0, chunks)
    def _(c):
        wait_for(r1.at[c], x_rcv.at[c])
        run_stages(r1.at[c], tmp, plan_t1)
        exchange(r1, r2, c, o1_snd, o1_rcv)

    start_gather(1, tb)
    load_a.wait()
    load_b.wait()

    @pl.loop(0, chunks)
    def _(c):
        wait_for(others(r2, c), o1_rcv.at[c])
        run_stages(r2.at[c], tmp, plan_n)
        exchange(r2, r3, c, i2_snd, i2_rcv)

    wait_gather(1, tb)

    @pl.loop(0, chunks)
    def _(c):
        wait_for(others(r3, c), i2_rcv.at[c])
        run_stages(r3.at[c], tmp, plan_t2)

        @pl.loop(0, n - 1)
        def _(t):
            d = peer(t)
            pltpu.make_async_remote_copy(
                src_ref=r3.at[c, mine(d)], dst_ref=out.at[mine(me), :, cols(c)],
                send_sem=o2_snd.at[c], recv_sem=o2_rcv.at[c],
                device_id={"sp": d}, device_id_type=MESH).start()

        pltpu.make_async_copy(r3.at[c, mine(me)], out.at[mine(me), :, cols(c)], o2_rcv.at[c]).start()

    @pl.loop(0, chunks)
    def _(c):
        wait_for(others(r1, c), x_snd.at[c])
        wait_for(others(r1, c), o1_snd.at[c])
        wait_for(others(r2, c), i2_snd.at[c])
        wait_for(others(r3, c), o2_snd.at[c])
        wait_for(out.at[:, :, cols(c)], o2_rcv.at[c])

    for m, t_buf in enumerate((ta, tb)):
        for q in range(units):
            s, l0 = item_of(my_part, q)
            wait_for(t_buf.at[s, pl.ds(0, n - 1), pl.ds(l0, unit)], z_snd.at[m, q])
            for k in range(1, sub):
                gather_copy(m, t_buf, k, q).wait_send()


def solution(mesh):
    n = mesh.shape["sp"]
    groups = mesh.shape["dp"]

    def pair_weights(w, distances):
        blocks = w.shape[1]
        index = lax.axis_index("sp") * blocks + jnp.arange(blocks)
        upper = jnp.stack([(index // d) % 2 for d in distances]) == 1
        own, cross = w[:, :, 0], w[:, :, 1]
        upper = upper[:, :, None, None]
        return jnp.concatenate([jnp.where(upper, cross, own), jnp.where(upper, own, cross)], axis=-1)

    def device_program(signal, w_first, w_second):
        stages, blocks, rows = w_first.shape[0], w_first.shape[1], w_first.shape[3]
        channels = signal.shape[1]
        chunks = channels // CHUNK
        cross = int(math.log2(n))
        local = stages - cross
        per = blocks // n
        sub = math.gcd(groups, cross * per)
        items = cross * per // sub
        units = items // min(items, per)
        down = [2 ** (stages - 1 - level) for level in range(stages)]
        wa = pair_weights(w_first, down)
        wb = pair_weights(w_second, down[::-1])
        x = signal.reshape(blocks, rows, channels)
        dma = pltpu.SemaphoreType.DMA
        buffer = pltpu.VMEM((chunks, blocks, rows, CHUNK), BF16)
        result = pl.pallas_call(
            functools.partial(kernel, n, groups, sub),
            out_shape=jax.ShapeDtypeStruct(x.shape, BF16),
            in_specs=[pl.BlockSpec(memory_space=pl.ANY)] * 3,
            out_specs=pl.BlockSpec(memory_space=pl.ANY),
            scratch_shapes=[
                buffer, buffer, buffer,
                pltpu.VMEM((blocks, rows, CHUNK), BF16),
                pltpu.VMEM((cross, n, per, rows, 2 * rows), BF16),
                pltpu.VMEM((cross, n, per, rows, 2 * rows), BF16),
                pltpu.VMEM((local, blocks, rows, 2 * rows), BF16),
                pltpu.VMEM((local, blocks, rows, 2 * rows), BF16),
                dma((chunks,)), dma((chunks,)), dma((chunks,)), dma((chunks,)),
                dma((chunks,)), dma((chunks,)), dma((chunks,)), dma((chunks,)),
                dma((2, units)), dma((2, units)), dma((2, sub, units)), dma((2, sub, units)),
                dma((2,)),
            ],
            compiler_params=pltpu.CompilerParams(
                collective_id=0, has_side_effects=True, vmem_limit_bytes=60 * 2 ** 20),
        )(x, wa, wb)
        return result.reshape(signal.shape)

    row_spec = P(("dp", "sp"), None)
    weight_spec = P(None, "sp", None, None, None)
    return jax.shard_map(device_program, mesh=mesh, in_specs=(row_spec, weight_spec, weight_spec), out_specs=row_spec, check_vma=False)
```

```python
import functools
import math

import jax
import jax.numpy as jnp
from jax import lax
from jax.experimental import pallas as pl
from jax.experimental.pallas import tpu as pltpu
from jax.sharding import PartitionSpec as P

MESH = pl.DeviceIdType.MESH
BF16 = jnp.bfloat16
F32 = jnp.float32
CHUNK = 256
UNROLL = 8
CORES = 2


def gelu(x):
    return 0.5 * x * (1.0 + lax.erf(x * (0.5 ** 0.5)))


def mix_stage(src, dst, weights, step, act):
    pairs = src.shape[0] // 2
    unroll = min(UNROLL, pairs)

    @pl.loop(0, pairs // unroll)
    def _(it):
        for u in range(unroll):
            p = it * unroll + u
            i = (p // step) * (2 * step) + p % step
            j = i + step
            z = jnp.concatenate([src[i], src[j]], axis=0)
            w = jnp.concatenate([weights(i), weights(j)], axis=0)
            o = jnp.dot(w, z, preferred_element_type=F32).astype(BF16)
            if act:
                o = gelu(o.astype(F32)).astype(BF16)
            half = o.shape[0] // 2
            dst[i] = o[:half]
            dst[j] = o[half:]


def partner_stage(own, other, dst, weights):
    blocks = own.shape[0]
    unroll = min(UNROLL, blocks)

    @pl.loop(0, blocks // unroll)
    def _(it):
        for u in range(unroll):
            i = it * unroll + u
            z = jnp.concatenate([own[i], other[i]], axis=0)
            dst[i] = jnp.dot(weights(i), z, preferred_element_type=F32).astype(BF16)


def kernel(n, sub, x, wa, wb, out, r1, r2, r3, rp, tmp, tmq, ta, tb, la, lb, wz, raw,
           x_snd, x_rcv, o1_snd, o1_rcv, i2_snd, i2_rcv, o2_snd, o2_rcv, p_snd, p_rcv,
           z_snd, z_rcv, g_snd, g_rcv, raw_sem):
    me = lax.axis_index("sp")
    dp = lax.axis_index("dp")
    chip, core = me // CORES, me % CORES
    partner = {"sp": me + 1 - 2 * core}
    part = dp % sub
    base = dp - part
    chunks, blocks = r1.shape[0], r1.shape[1]
    stages = wa.shape[0]
    chips = n // CORES
    far = ta.shape[0]
    near = stages - far
    per = blocks // chips
    take = per // sub
    mine_l = pl.ds(part * take, take)

    def peer(t):
        side = 1 - 2 * (t % 2)
        return (chip + chips // 2 + side * ((t + 1) // 2) + chips) % chips

    def on(z):
        return {"sp": z * CORES + core}

    def group(k):
        return {"dp": base + (part + k) % sub}

    def cols(c):
        return pl.ds(pl.multiple_of(c * CHUNK, CHUNK), CHUNK)

    def of(z):
        return pl.ds(z * per, per)

    def wait_for(ref, sem):
        pltpu.make_async_copy(ref, ref, sem).wait()

    barrier = pltpu.get_barrier_semaphore()

    @pl.loop(0, chips - 1)
    def _(t):
        pl.semaphore_signal(barrier, inc=1, device_id=on(peer(t)), device_id_type=MESH)

    pl.semaphore_signal(barrier, inc=1, device_id=partner, device_id_type=MESH)
    for k in range(1, sub):
        pl.semaphore_signal(barrier, inc=1, device_id=group(k), device_id_type=MESH)
    pl.semaphore_wait(barrier, chips + sub - 1)

    jobs = [(m, s, True) for m in range(2) for s in range(far)]
    jobs += [(m, s, False) for m in range(2) for s in range(near)]
    w_of, t_of, l_of = (wa, wb), (ta, tb), (la, lb)

    def load(job):
        m, s, is_far = jobs[job]
        slot = job % 2
        if is_far:
            src = w_of[m].at[(0, near)[m] + s, :, mine_l]
            dst = raw.at[slot, :, pl.ds(0, take)]
        else:
            src, dst = w_of[m].at[(far, 0)[m] + s], raw.at[slot]
        return pltpu.make_async_copy(src, dst, raw_sem.at[slot])

    def prepare(job):
        m, s, is_far = jobs[job]
        slot = job % 2
        if is_far:
            upper = (chip // 2 ** (far - 1 - s, s)[m]) % 2 == 1

            @pl.loop(0, chips)
            def _(z):
                for b in range(take):
                    own, cross = raw[slot, z, b, 0], raw[slot, z, b, 1]
                    left, right = jnp.where(upper, cross, own), jnp.where(upper, own, cross)
                    wz[m, s, z, b] = jnp.concatenate([left, right], axis=-1)
        else:
            level = (near - 1 - s, s)[m]
            step = 2 ** level

            @pl.loop(0, blocks // 8)
            def _(it):
                for u in range(4):
                    p = it * 4 + u
                    i = (p // step) * (2 * step) + p % step
                    j = i + step
                    if level == near - 1:
                        i, j, swap = 2 * p, 2 * p + 1, False
                    else:
                        swap = True
                    first = [raw[slot, i // per, i % per, h] for h in range(2)]
                    second = [raw[slot, j // per, j % per, h] for h in range(2)]
                    l_of[m][s, i] = jnp.concatenate(first, axis=-1)
                    l_of[m][s, j] = jnp.concatenate(second[::-1] if swap else second, axis=-1)

    def run_jobs(first, last):
        for job in range(first, last):
            load(job).wait()
            prepare(job)
            if job + 2 < len(jobs):
                load(job + 2).start()

    def send_weights(m):
        @pl.loop(0, chips - 1)
        def _(t):
            z = peer(t)
            pltpu.make_async_remote_copy(
                src_ref=wz.at[m, :, z], dst_ref=t_of[m].at[:, chip, mine_l],
                send_sem=z_snd.at[m], recv_sem=z_rcv.at[m],
                device_id=on(z), device_id_type=MESH).start()

        for s in range(far):
            for b in range(take):
                t_of[m][s, chip, part * take + b] = wz[m, s, chip, b]

    def gather_copy(m, k):
        ref = t_of[m].at[:, :, mine_l]
        return pltpu.make_async_remote_copy(
            src_ref=ref, dst_ref=ref, send_sem=g_snd.at[m, k], recv_sem=g_rcv.at[m, k],
            device_id=group(k), device_id_type=MESH)

    def start_gather(m):
        wait_for(t_of[m].at[:, pl.ds(0, chips - 1), mine_l], z_rcv.at[m])
        for k in range(1, sub):
            gather_copy(m, k).start()

    def wait_gather(m):
        for k in range(1, sub):
            theirs = (part - k + sub) % sub
            wait_for(t_of[m].at[:, :, pl.ds(theirs * take, take)], g_rcv.at[m, k])

    def send_signal(c):
        @pl.loop(0, chips - 1)
        def _(t):
            z = peer(t)
            pltpu.make_async_remote_copy(
                src_ref=x.at[of(z), :, cols(c)], dst_ref=r1.at[c, of(chip)],
                send_sem=x_snd.at[c], recv_sem=x_rcv.at[c],
                device_id=on(z), device_id_type=MESH).start()

        pltpu.make_async_copy(x.at[of(chip), :, cols(c)], r1.at[c, of(chip)], x_rcv.at[c]).start()

    load(0).start()
    load(1).start()
    send_signal(0)
    run_jobs(0, far)
    send_weights(0)

    @pl.loop(1, chunks)
    def _(c):
        send_signal(c)

    run_jobs(far, 2 * far)
    send_weights(1)
    run_jobs(2 * far, len(jobs))
    start_gather(0)
    wait_gather(0)

    def far_weights(m, s):
        return lambda i: t_of[m][s, i // per, i % per]

    def near_weights(m, s):
        return lambda i: l_of[m][s, i]

    far_steps = [per * 2 ** s for s in range(far)]
    plan_t1 = [(far_weights(0, s), step, False) for s, step in enumerate(far_steps[::-1])]
    plan_t2 = [(far_weights(1, s), step, False) for s, step in enumerate(far_steps)]
    near_steps = [2 ** s for s in range(near - 1)]
    plan_n = [(near_weights(0, s + 1), step, step == 1) for s, step in enumerate(near_steps[::-1])]
    plan_n += [(near_weights(1, s), step, False) for s, step in enumerate(near_steps)]

    def run_far(buf, plan):
        src = buf
        for k, (weights, step, act) in enumerate(plan):
            dst = buf if k == len(plan) - 1 else (tmp, tmq)[k % 2]
            mix_stage(src, dst, weights, step, act)
            src = dst

    def others(ref, c):
        return ref.at[c, pl.ds(0, (chips - 1) * per)]

    def exchange(src, dst, c, snd, rcv):
        @pl.loop(0, chips - 1)
        def _(t):
            z = peer(t)
            pltpu.make_async_remote_copy(
                src_ref=src.at[c, of(z)], dst_ref=dst.at[c, of(chip)],
                send_sem=snd.at[c], recv_sem=rcv.at[c],
                device_id=on(z), device_id_type=MESH).start()

        dst[c, of(chip)] = src[c, of(chip)]

    @pl.loop(0, chunks)
    def _(c):
        wait_for(r1.at[c], x_rcv.at[c])
        run_far(r1.at[c], plan_t1)
        exchange(r1, r2, c, o1_snd, o1_rcv)

    start_gather(1)

    def partner_copy(k, src, dst, c):
        return pltpu.make_async_remote_copy(
            src_ref=src, dst_ref=dst, send_sem=p_snd.at[k, c], recv_sem=p_rcv.at[k, c],
            device_id=partner, device_id_type=MESH)

    @pl.loop(0, chunks)
    def _(c):
        wait_for(others(r2, c), o1_rcv.at[c])
        wait_for(others(r1, c), o1_snd.at[c])
        copy = partner_copy(0, r2.at[c], rp.at[c], c)
        copy.start()
        copy.wait_recv()
        partner_stage(r2.at[c], rp.at[c], tmp, near_weights(0, 0))
        copy.wait_send()
        src, dst = tmp, r2.at[c]
        for weights, step, act in plan_n:
            mix_stage(src, dst, weights, step, act)
            src, dst = dst, src
        copy = partner_copy(1, tmp, r1.at[c], c)
        copy.start()
        copy.wait_recv()
        partner_stage(tmp, r1.at[c], r2.at[c], near_weights(1, near - 1))
        copy.wait_send()
        exchange(r2, r3, c, i2_snd, i2_rcv)

    wait_gather(1)

    @pl.loop(0, chunks)
    def _(c):
        wait_for(others(r3, c), i2_rcv.at[c])
        run_far(r3.at[c], plan_t2)

        @pl.loop(0, chips - 1)
        def _(t):
            z = peer(t)
            pltpu.make_async_remote_copy(
                src_ref=r3.at[c, of(z)], dst_ref=out.at[of(chip), :, cols(c)],
                send_sem=o2_snd.at[c], recv_sem=o2_rcv.at[c],
                device_id=on(z), device_id_type=MESH).start()

        pltpu.make_async_copy(r3.at[c, of(chip)], out.at[of(chip), :, cols(c)], o2_rcv.at[c]).start()

    for m in range(2):
        wait_for(t_of[m].at[:, pl.ds(0, chips - 1), mine_l], z_snd.at[m])
        for k in range(1, sub):
            gather_copy(m, k).wait_send()

    @pl.loop(0, chunks)
    def _(c):
        wait_for(others(r1, c), x_snd.at[c])
        wait_for(others(r2, c), i2_snd.at[c])
        wait_for(others(r3, c), o2_snd.at[c])
        wait_for(out.at[:, :, cols(c)], o2_rcv.at[c])


def solution(mesh):
    n = mesh.shape["sp"]
    groups = mesh.shape["dp"]
    chips = n // CORES
    far = int(math.log2(chips))

    def device_program(signal, w_first, w_second):
        stages, blocks, _, rows, _ = w_first.shape
        channels = signal.shape[1]
        chunks = channels // CHUNK
        near = stages - far
        per = blocks // chips
        sub = math.gcd(groups, per)
        x = signal.reshape(blocks, rows, channels)
        by_chip = (stages, chips, per, 2, rows, rows)
        dma = pltpu.SemaphoreType.DMA
        buffer = pltpu.VMEM((chunks, blocks, rows, CHUNK), BF16)
        temp = pltpu.VMEM((blocks, rows, CHUNK), BF16)
        far_w = pltpu.VMEM((far, chips, per, rows, 2 * rows), BF16)
        near_w = pltpu.VMEM((near, blocks, rows, 2 * rows), BF16)
        result = pl.pallas_call(
            functools.partial(kernel, n, sub),
            out_shape=jax.ShapeDtypeStruct(x.shape, BF16),
            in_specs=[pl.BlockSpec(memory_space=pl.ANY)] * 3,
            out_specs=pl.BlockSpec(memory_space=pl.ANY),
            scratch_shapes=[
                buffer, buffer, buffer, buffer, temp, temp, far_w, far_w, near_w, near_w,
                pltpu.VMEM((2, far, chips, per // sub, rows, 2 * rows), BF16),
                pltpu.VMEM((2, chips, per, 2, rows, rows), BF16),
                dma((chunks,)), dma((chunks,)), dma((chunks,)), dma((chunks,)),
                dma((chunks,)), dma((chunks,)), dma((chunks,)), dma((chunks,)),
                dma((2, chunks)), dma((2, chunks)),
                dma((2,)), dma((2,)), dma((2, sub)), dma((2, sub)),
                dma((2,)),
            ],
            compiler_params=pltpu.CompilerParams(
                collective_id=0, has_side_effects=True, vmem_limit_bytes=62 * 2 ** 20),
        )(x, w_first.reshape(by_chip), w_second.reshape(by_chip))
        return result.reshape(signal.shape)

    row_spec = P(("dp", "sp"), None)
    weight_spec = P(None, "sp", None, None, None)
    return jax.shard_map(device_program, mesh=mesh, in_specs=(row_spec, weight_spec, weight_spec), out_specs=row_spec, check_vma=False)
```

```python
import functools
import math

import jax
import jax.numpy as jnp
from jax import lax
from jax.experimental import pallas as pl
from jax.experimental.pallas import tpu as pltpu
from jax.sharding import PartitionSpec as P

MESH = pl.DeviceIdType.MESH
BF16 = jnp.bfloat16
F32 = jnp.float32
CHUNK = 256
UNROLL = 8
CORES = 2


def gelu(x):
    return 0.5 * x * (1.0 + lax.erf(x * (0.5 ** 0.5)))


def mix_stage(src, dst, weights, step, act):
    pairs = src.shape[0] // 2
    unroll = min(UNROLL, pairs)

    @pl.loop(0, pairs // unroll)
    def _(it):
        for u in range(unroll):
            p = it * unroll + u
            i = (p // step) * (2 * step) + p % step
            j = i + step
            z = jnp.concatenate([src[i], src[j]], axis=0)
            w = jnp.concatenate([weights(i), weights(j)], axis=0)
            o = jnp.dot(w, z, preferred_element_type=F32).astype(BF16)
            if act:
                o = gelu(o.astype(F32)).astype(BF16)
            half = o.shape[0] // 2
            dst[i] = o[:half]
            dst[j] = o[half:]


def partner_stage(own, other, dst, weights):
    blocks = own.shape[0]
    unroll = min(UNROLL, blocks)

    @pl.loop(0, blocks // unroll)
    def _(it):
        for u in range(unroll):
            i = it * unroll + u
            z = jnp.concatenate([own[i], other[i]], axis=0)
            dst[i] = jnp.dot(weights(i), z, preferred_element_type=F32).astype(BF16)


def kernel(n, sub, x, wa, wb, out, r1, r2, r3, rp, tmp, tmq, ta, tb, la, lb, wz, raw,
           x_snd, x_rcv, o1_snd, o1_rcv, i2_snd, i2_rcv, o2_snd, o2_rcv, p_snd, p_rcv,
           z_snd, z_rcv, g_snd, g_rcv, raw_sem):
    me = lax.axis_index("sp")
    dp = lax.axis_index("dp")
    chip, core = me // CORES, me % CORES
    partner = {"sp": me + 1 - 2 * core}
    part = dp % sub
    base = dp - part
    chunks, blocks = r1.shape[0], r1.shape[1]
    stages = wa.shape[0]
    chips = n // CORES
    far = ta.shape[0]
    near = stages - far
    per = blocks // chips
    take = per // sub
    mine_l = pl.ds(part * take, take)

    def peer(t):
        side = 1 - 2 * (t % 2)
        return (chip + chips // 2 + side * ((t + 1) // 2) + chips) % chips

    def on(z):
        return {"sp": z * CORES + core}

    def group(k):
        return {"dp": base + (part + k) % sub}

    def cols(c):
        return pl.ds(pl.multiple_of(c * CHUNK, CHUNK), CHUNK)

    def of(z):
        return pl.ds(z * per, per)

    def wait_for(ref, sem):
        pltpu.make_async_copy(ref, ref, sem).wait()

    barrier = pltpu.get_barrier_semaphore()

    @pl.loop(0, chips - 1)
    def _(t):
        pl.semaphore_signal(barrier, inc=1, device_id=on(peer(t)), device_id_type=MESH)

    pl.semaphore_signal(barrier, inc=1, device_id=partner, device_id_type=MESH)
    for k in range(1, sub):
        pl.semaphore_signal(barrier, inc=1, device_id=group(k), device_id_type=MESH)
    pl.semaphore_wait(barrier, chips + sub - 1)

    jobs = [(m, s, True) for m in range(2) for s in range(far)]
    jobs += [(m, s, False) for m in range(2) for s in range(near)]
    w_of, t_of, l_of = (wa, wb), (ta, tb), (la, lb)

    def load(job):
        m, s, is_far = jobs[job]
        slot = job % 2
        if is_far:
            src = w_of[m].at[(0, near)[m] + s, :, mine_l]
            dst = raw.at[slot, :, pl.ds(0, take)]
        else:
            src, dst = w_of[m].at[(far, 0)[m] + s], raw.at[slot]
        return pltpu.make_async_copy(src, dst, raw_sem.at[slot])

    def prepare(job):
        m, s, is_far = jobs[job]
        slot = job % 2
        if is_far:
            upper = (chip // 2 ** (far - 1 - s, s)[m]) % 2 == 1

            @pl.loop(0, chips)
            def _(z):
                for b in range(take):
                    own, cross = raw[slot, z, b, 0], raw[slot, z, b, 1]
                    left, right = jnp.where(upper, cross, own), jnp.where(upper, own, cross)
                    wz[m, s, z, b] = jnp.concatenate([left, right], axis=-1)
        else:
            level = (near - 1 - s, s)[m]
            step = 2 ** level

            @pl.loop(0, blocks // 8)
            def _(it):
                for u in range(4):
                    p = it * 4 + u
                    i = (p // step) * (2 * step) + p % step
                    j = i + step
                    if level == near - 1:
                        i, j, swap = 2 * p, 2 * p + 1, False
                    else:
                        swap = True
                    first = [raw[slot, i // per, i % per, h] for h in range(2)]
                    second = [raw[slot, j // per, j % per, h] for h in range(2)]
                    l_of[m][s, i] = jnp.concatenate(first, axis=-1)
                    l_of[m][s, j] = jnp.concatenate(second[::-1] if swap else second, axis=-1)

    def run_jobs(first, last):
        for job in range(first, last):
            load(job).wait()
            prepare(job)
            if job + 2 < len(jobs):
                load(job + 2).start()

    def send_weights(m):
        @pl.loop(0, chips - 1)
        def _(t):
            z = peer(t)
            pltpu.make_async_remote_copy(
                src_ref=wz.at[m, :, z], dst_ref=t_of[m].at[:, chip, mine_l],
                send_sem=z_snd.at[m], recv_sem=z_rcv.at[m],
                device_id=on(z), device_id_type=MESH).start()

        for s in range(far):
            for b in range(take):
                t_of[m][s, chip, part * take + b] = wz[m, s, chip, b]

    def gather_copy(m, k):
        ref = t_of[m].at[:, :, mine_l]
        return pltpu.make_async_remote_copy(
            src_ref=ref, dst_ref=ref, send_sem=g_snd.at[m, k], recv_sem=g_rcv.at[m, k],
            device_id=group(k), device_id_type=MESH)

    def start_gather(m):
        wait_for(t_of[m].at[:, pl.ds(0, chips - 1), mine_l], z_rcv.at[m])
        for k in range(1, sub):
            gather_copy(m, k).start()

    def wait_gather(m):
        for k in range(1, sub):
            theirs = (part - k + sub) % sub
            wait_for(t_of[m].at[:, :, pl.ds(theirs * take, take)], g_rcv.at[m, k])

    def send_signal(c):
        @pl.loop(0, chips - 1)
        def _(t):
            z = peer(t)
            pltpu.make_async_remote_copy(
                src_ref=x.at[of(z), :, cols(c)], dst_ref=r1.at[c, of(chip)],
                send_sem=x_snd.at[c], recv_sem=x_rcv.at[c],
                device_id=on(z), device_id_type=MESH).start()

        pltpu.make_async_copy(x.at[of(chip), :, cols(c)], r1.at[c, of(chip)], x_rcv.at[c]).start()

    load(0).start()
    load(1).start()
    send_signal(0)
    run_jobs(0, far)
    send_weights(0)

    @pl.loop(1, chunks)
    def _(c):
        send_signal(c)

    run_jobs(far, 2 * far)
    send_weights(1)
    run_jobs(2 * far, len(jobs))
    start_gather(0)
    wait_gather(0)

    def far_weights(m, s):
        return lambda i: t_of[m][s, i // per, i % per]

    def near_weights(m, s):
        return lambda i: l_of[m][s, i]

    far_steps = [per * 2 ** s for s in range(far)]
    plan_t1 = [(far_weights(0, s), step, False) for s, step in enumerate(far_steps[::-1])]
    plan_t2 = [(far_weights(1, s), step, False) for s, step in enumerate(far_steps)]
    near_steps = [2 ** s for s in range(near - 1)]
    plan_n = [(near_weights(0, s + 1), step, step == 1) for s, step in enumerate(near_steps[::-1])]
    plan_n += [(near_weights(1, s), step, False) for s, step in enumerate(near_steps)]

    def run_far(buf, plan):
        src = buf
        for k, (weights, step, act) in enumerate(plan):
            dst = buf if k == len(plan) - 1 else (tmp, tmq)[k % 2]
            mix_stage(src, dst, weights, step, act)
            src = dst

    def others(ref, c):
        return ref.at[c, pl.ds(0, (chips - 1) * per)]

    def exchange(src, dst, c, snd, rcv):
        @pl.loop(0, chips - 1)
        def _(t):
            z = peer(t)
            pltpu.make_async_remote_copy(
                src_ref=src.at[c, of(z)], dst_ref=dst.at[c, of(chip)],
                send_sem=snd.at[c], recv_sem=rcv.at[c],
                device_id=on(z), device_id_type=MESH).start()

        dst[c, of(chip)] = src[c, of(chip)]

    @pl.loop(0, chunks)
    def _(c):
        wait_for(r1.at[c], x_rcv.at[c])
        run_far(r1.at[c], plan_t1)
        exchange(r1, r2, c, o1_snd, o1_rcv)

    start_gather(1)

    def partner_copy(k, src, dst, c):
        return pltpu.make_async_remote_copy(
            src_ref=src, dst_ref=dst, send_sem=p_snd.at[k, c], recv_sem=p_rcv.at[k, c],
            device_id=partner, device_id_type=MESH)

    @pl.loop(0, chunks)
    def _(c):
        wait_for(others(r2, c), o1_rcv.at[c])
        wait_for(others(r1, c), o1_snd.at[c])
        copy = partner_copy(0, r2.at[c], rp.at[c], c)
        copy.start()
        copy.wait_recv()
        partner_stage(r2.at[c], rp.at[c], tmp, near_weights(0, 0))
        copy.wait_send()
        src, dst = tmp, r2.at[c]
        for weights, step, act in plan_n:
            mix_stage(src, dst, weights, step, act)
            src, dst = dst, src
        copy = partner_copy(1, tmp, r1.at[c], c)
        copy.start()
        copy.wait_recv()
        partner_stage(tmp, r1.at[c], r2.at[c], near_weights(1, near - 1))
        copy.wait_send()
        exchange(r2, r3, c, i2_snd, i2_rcv)

    wait_gather(1)

    @pl.loop(0, chunks)
    def _(c):
        wait_for(others(r3, c), i2_rcv.at[c])
        run_far(r3.at[c], plan_t2)

        @pl.loop(0, chips - 1)
        def _(t):
            z = peer(t)
            pltpu.make_async_remote_copy(
                src_ref=r3.at[c, of(z)], dst_ref=out.at[of(chip), :, cols(c)],
                send_sem=o2_snd.at[c], recv_sem=o2_rcv.at[c],
                device_id=on(z), device_id_type=MESH).start()

        out[of(chip), :, cols(c)] = r3[c, of(chip)]

    for m in range(2):
        wait_for(t_of[m].at[:, pl.ds(0, chips - 1), mine_l], z_snd.at[m])
        for k in range(1, sub):
            gather_copy(m, k).wait_send()

    @pl.loop(0, chunks)
    def _(c):
        wait_for(others(r1, c), x_snd.at[c])
        wait_for(others(r2, c), i2_snd.at[c])
        wait_for(others(r3, c), o2_snd.at[c])
        wait_for(out.at[pl.ds(0, (chips - 1) * per), :, cols(c)], o2_rcv.at[c])


def solution(mesh):
    n = mesh.shape["sp"]
    groups = mesh.shape["dp"]
    chips = n // CORES
    far = int(math.log2(chips))

    def device_program(signal, w_first, w_second):
        stages, blocks, _, rows, _ = w_first.shape
        channels = signal.shape[1]
        chunks = channels // CHUNK
        near = stages - far
        per = blocks // chips
        sub = math.gcd(groups, per)
        x = signal.reshape(blocks, rows, channels)
        by_chip = (stages, chips, per, 2, rows, rows)
        dma = pltpu.SemaphoreType.DMA
        buffer = pltpu.VMEM((chunks, blocks, rows, CHUNK), BF16)
        temp = pltpu.VMEM((blocks, rows, CHUNK), BF16)
        far_w = pltpu.VMEM((far, chips, per, rows, 2 * rows), BF16)
        near_w = pltpu.VMEM((near, blocks, rows, 2 * rows), BF16)
        result = pl.pallas_call(
            functools.partial(kernel, n, sub),
            out_shape=pltpu.VMEM(x.shape, BF16),
            in_specs=[pl.BlockSpec(memory_space=pl.ANY)] * 3,
            out_specs=pl.BlockSpec(memory_space=pltpu.VMEM),
            scratch_shapes=[
                buffer, buffer, buffer, buffer, temp, temp, far_w, far_w, near_w, near_w,
                pltpu.VMEM((2, far, chips, per // sub, rows, 2 * rows), BF16),
                pltpu.VMEM((2, chips, per, 2, rows, rows), BF16),
                dma((chunks,)), dma((chunks,)), dma((chunks,)), dma((chunks,)),
                dma((chunks,)), dma((chunks,)), dma((chunks,)), dma((chunks,)),
                dma((2, chunks)), dma((2, chunks)),
                dma((2,)), dma((2,)), dma((2, sub)), dma((2, sub)),
                dma((2,)),
            ],
            compiler_params=pltpu.CompilerParams(
                collective_id=0, has_side_effects=True, vmem_limit_bytes=56 * 2 ** 20),
        )(x, w_first.reshape(by_chip), w_second.reshape(by_chip))
        return result.reshape(signal.shape)

    row_spec = P(("dp", "sp"), None)
    weight_spec = P(None, "sp", None, None, None)
    return jax.shard_map(device_program, mesh=mesh, in_specs=(row_spec, weight_spec, weight_spec), out_specs=row_spec, check_vma=False)
```

```python
import functools
import math

import jax
import jax.numpy as jnp
from jax import lax
from jax.experimental import pallas as pl
from jax.experimental.pallas import tpu as pltpu
from jax.sharding import PartitionSpec as P

MESH = pl.DeviceIdType.MESH
BF16 = jnp.bfloat16
F32 = jnp.float32
CHUNK = 256
UNROLL = 8
CORES = 2


def gelu(x):
    return 0.5 * x * (1.0 + lax.erf(x * (0.5 ** 0.5)))


def mix_stage(src, dst, weights, step, act):
    pairs = src.shape[0] // 2
    unroll = min(UNROLL, pairs)

    @pl.loop(0, pairs // unroll)
    def _(it):
        for u in range(unroll):
            p = it * unroll + u
            i = (p // step) * (2 * step) + p % step
            j = i + step
            z = jnp.concatenate([src[i], src[j]], axis=0)
            w = jnp.concatenate([weights(i), weights(j)], axis=0)
            o = jnp.dot(w, z, preferred_element_type=F32).astype(BF16)
            if act:
                o = gelu(o.astype(F32)).astype(BF16)
            half = o.shape[0] // 2
            dst[i] = o[:half]
            dst[j] = o[half:]


def partner_stage(own, other, dst, weights):
    blocks = own.shape[0]
    unroll = min(UNROLL, blocks)

    @pl.loop(0, blocks // unroll)
    def _(it):
        for u in range(unroll):
            i = it * unroll + u
            z = jnp.concatenate([own[i], other[i]], axis=0)
            dst[i] = jnp.dot(weights(i), z, preferred_element_type=F32).astype(BF16)


def kernel(n, sub, x, wa, wb, out, r1, r2, r3, rp, tmp, tmq, ta, tb, la, lb, wz, raw,
           x_snd, x_rcv, o1_snd, o1_rcv, i2_snd, i2_rcv, o2_snd, o2_rcv, p_snd, p_rcv,
           z_snd, z_rcv, g_snd, g_rcv, raw_sem):
    me = lax.axis_index("sp")
    dp = lax.axis_index("dp")
    chip, core = me // CORES, me % CORES
    partner = {"sp": me + 1 - 2 * core}
    part = dp % sub
    base = dp - part
    chunks, blocks = r1.shape[0], r1.shape[1]
    stages = wa.shape[0]
    chips = n // CORES
    far = ta.shape[0]
    near = stages - far
    per = blocks // chips
    take = per // sub
    mine_l = pl.ds(part * take, take)

    def peer(t):
        if chips == 2:
            return (chip + 1) % chips
        pair, last = t // 2, t // (chips - 2)
        reach = chips // 2 - 1
        distance = (reach - pair) + core * (2 * pair + 1 - reach)
        offset = distance + (t % 2) * (chips - 2 * distance)
        return (chip + last * (chips // 2) + (1 - last) * offset) % chips

    def on(z):
        return {"sp": z * CORES + core}

    def group(k):
        return {"dp": base + (part + k) % sub}

    def cols(c):
        return pl.ds(pl.multiple_of(c * CHUNK, CHUNK), CHUNK)

    def of(z):
        return pl.ds(z * per, per)

    def wait_for(ref, sem):
        pltpu.make_async_copy(ref, ref, sem).wait()

    barrier = pltpu.get_barrier_semaphore()

    @pl.loop(0, chips - 1)
    def _(t):
        pl.semaphore_signal(barrier, inc=1, device_id=on(peer(t)), device_id_type=MESH)

    pl.semaphore_signal(barrier, inc=1, device_id=partner, device_id_type=MESH)
    for k in range(1, sub):
        pl.semaphore_signal(barrier, inc=1, device_id=group(k), device_id_type=MESH)
    pl.semaphore_wait(barrier, chips + sub - 1)

    jobs = [(m, s, True) for m in range(2) for s in range(far)]
    jobs += [(m, s, False) for m in range(2) for s in range(near)]
    w_of, t_of, l_of = (wa, wb), (ta, tb), (la, lb)

    def load(job):
        m, s, is_far = jobs[job]
        slot = job % 2
        if is_far:
            src = w_of[m].at[(0, near)[m] + s, :, mine_l]
            dst = raw.at[slot, :, pl.ds(0, take)]
        else:
            src, dst = w_of[m].at[(far, 0)[m] + s], raw.at[slot]
        return pltpu.make_async_copy(src, dst, raw_sem.at[slot])

    def prepare(job):
        m, s, is_far = jobs[job]
        slot = job % 2
        if is_far:
            upper = (chip // 2 ** (far - 1 - s, s)[m]) % 2 == 1

            @pl.loop(0, chips)
            def _(z):
                for b in range(take):
                    own, cross = raw[slot, z, b, 0], raw[slot, z, b, 1]
                    left, right = jnp.where(upper, cross, own), jnp.where(upper, own, cross)
                    wz[m, s, z, b] = jnp.concatenate([left, right], axis=-1)
        else:
            level = (near - 1 - s, s)[m]
            step = 2 ** level

            @pl.loop(0, blocks // 8)
            def _(it):
                for u in range(4):
                    p = it * 4 + u
                    i = (p // step) * (2 * step) + p % step
                    j = i + step
                    if level == near - 1:
                        i, j, swap = 2 * p, 2 * p + 1, False
                    else:
                        swap = True
                    first = [raw[slot, i // per, i % per, h] for h in range(2)]
                    second = [raw[slot, j // per, j % per, h] for h in range(2)]
                    l_of[m][s, i] = jnp.concatenate(first, axis=-1)
                    l_of[m][s, j] = jnp.concatenate(second[::-1] if swap else second, axis=-1)

    def run_jobs(first, last):
        for job in range(first, last):
            load(job).wait()
            prepare(job)
            if job + 2 < len(jobs):
                load(job + 2).start()

    def send_weights(m):
        @pl.loop(0, chips - 1)
        def _(t):
            z = peer(t)
            pltpu.make_async_remote_copy(
                src_ref=wz.at[m, :, z], dst_ref=t_of[m].at[:, chip, mine_l],
                send_sem=z_snd.at[m], recv_sem=z_rcv.at[m],
                device_id=on(z), device_id_type=MESH).start()

        for s in range(far):
            for b in range(take):
                t_of[m][s, chip, part * take + b] = wz[m, s, chip, b]

    def gather_copy(m, k):
        ref = t_of[m].at[:, :, mine_l]
        return pltpu.make_async_remote_copy(
            src_ref=ref, dst_ref=ref, send_sem=g_snd.at[m, k], recv_sem=g_rcv.at[m, k],
            device_id=group(k), device_id_type=MESH)

    def start_gather(m):
        wait_for(t_of[m].at[:, pl.ds(0, chips - 1), mine_l], z_rcv.at[m])
        for k in range(1, sub):
            gather_copy(m, k).start()

    def wait_gather(m):
        for k in range(1, sub):
            theirs = (part - k + sub) % sub
            wait_for(t_of[m].at[:, :, pl.ds(theirs * take, take)], g_rcv.at[m, k])

    def send_signal(c):
        @pl.loop(0, chips - 1)
        def _(t):
            z = peer(t)
            pltpu.make_async_remote_copy(
                src_ref=x.at[of(z), :, cols(c)], dst_ref=r1.at[c, of(chip)],
                send_sem=x_snd.at[c], recv_sem=x_rcv.at[c],
                device_id=on(z), device_id_type=MESH).start()

        pltpu.make_async_copy(x.at[of(chip), :, cols(c)], r1.at[c, of(chip)], x_rcv.at[c]).start()

    load(0).start()
    load(1).start()
    send_signal(0)
    run_jobs(0, far)
    send_weights(0)

    @pl.loop(1, chunks)
    def _(c):
        send_signal(c)

    run_jobs(far, 2 * far)
    send_weights(1)
    run_jobs(2 * far, len(jobs))
    start_gather(0)
    wait_gather(0)

    def far_weights(m, s):
        return lambda i: t_of[m][s, i // per, i % per]

    def near_weights(m, s):
        return lambda i: l_of[m][s, i]

    far_steps = [per * 2 ** s for s in range(far)]
    plan_t1 = [(far_weights(0, s), step, False) for s, step in enumerate(far_steps[::-1])]
    plan_t2 = [(far_weights(1, s), step, False) for s, step in enumerate(far_steps)]
    near_steps = [2 ** s for s in range(near - 1)]
    plan_n = [(near_weights(0, s + 1), step, step == 1) for s, step in enumerate(near_steps[::-1])]
    plan_n += [(near_weights(1, s), step, False) for s, step in enumerate(near_steps)]

    def run_far(buf, plan):
        src = buf
        for k, (weights, step, act) in enumerate(plan):
            dst = buf if k == len(plan) - 1 else (tmp, tmq)[k % 2]
            mix_stage(src, dst, weights, step, act)
            src = dst

    def others(ref, c):
        return ref.at[c, pl.ds(0, (chips - 1) * per)]

    def exchange(src, dst, c, snd, rcv):
        @pl.loop(0, chips - 1)
        def _(t):
            z = peer(t)
            pltpu.make_async_remote_copy(
                src_ref=src.at[c, of(z)], dst_ref=dst.at[c, of(chip)],
                send_sem=snd.at[c], recv_sem=rcv.at[c],
                device_id=on(z), device_id_type=MESH).start()

        dst[c, of(chip)] = src[c, of(chip)]

    @pl.loop(0, chunks)
    def _(c):
        wait_for(r1.at[c], x_rcv.at[c])
        run_far(r1.at[c], plan_t1)
        exchange(r1, r2, c, o1_snd, o1_rcv)

    start_gather(1)

    def partner_copy(k, src, dst, c):
        return pltpu.make_async_remote_copy(
            src_ref=src, dst_ref=dst, send_sem=p_snd.at[k, c], recv_sem=p_rcv.at[k, c],
            device_id=partner, device_id_type=MESH)

    @pl.loop(0, chunks)
    def _(c):
        wait_for(others(r2, c), o1_rcv.at[c])
        wait_for(others(r1, c), o1_snd.at[c])
        copy = partner_copy(0, r2.at[c], rp.at[c], c)
        copy.start()
        copy.wait_recv()
        partner_stage(r2.at[c], rp.at[c], tmp, near_weights(0, 0))
        copy.wait_send()
        src, dst = tmp, r2.at[c]
        for weights, step, act in plan_n:
            mix_stage(src, dst, weights, step, act)
            src, dst = dst, src
        copy = partner_copy(1, tmp, r1.at[c], c)
        copy.start()
        copy.wait_recv()
        partner_stage(tmp, r1.at[c], r2.at[c], near_weights(1, near - 1))
        copy.wait_send()
        exchange(r2, r3, c, i2_snd, i2_rcv)

    wait_gather(1)

    @pl.loop(0, chunks)
    def _(c):
        wait_for(others(r3, c), i2_rcv.at[c])
        run_far(r3.at[c], plan_t2)

        @pl.loop(0, chips - 1)
        def _(t):
            z = peer(t)
            pltpu.make_async_remote_copy(
                src_ref=r3.at[c, of(z)], dst_ref=out.at[of(chip), :, cols(c)],
                send_sem=o2_snd.at[c], recv_sem=o2_rcv.at[c],
                device_id=on(z), device_id_type=MESH).start()

        out[of(chip), :, cols(c)] = r3[c, of(chip)]

    for m in range(2):
        wait_for(t_of[m].at[:, pl.ds(0, chips - 1), mine_l], z_snd.at[m])
        for k in range(1, sub):
            gather_copy(m, k).wait_send()

    @pl.loop(0, chunks)
    def _(c):
        wait_for(others(r1, c), x_snd.at[c])
        wait_for(others(r2, c), i2_snd.at[c])
        wait_for(others(r3, c), o2_snd.at[c])
        wait_for(out.at[pl.ds(0, (chips - 1) * per), :, cols(c)], o2_rcv.at[c])


def solution(mesh):
    n = mesh.shape["sp"]
    groups = mesh.shape["dp"]
    chips = n // CORES
    far = int(math.log2(chips))

    def device_program(signal, w_first, w_second):
        stages, blocks, _, rows, _ = w_first.shape
        channels = signal.shape[1]
        chunks = channels // CHUNK
        near = stages - far
        per = blocks // chips
        sub = math.gcd(groups, per)
        x = signal.reshape(blocks, rows, channels)
        by_chip = (stages, chips, per, 2, rows, rows)
        dma = pltpu.SemaphoreType.DMA
        buffer = pltpu.VMEM((chunks, blocks, rows, CHUNK), BF16)
        temp = pltpu.VMEM((blocks, rows, CHUNK), BF16)
        far_w = pltpu.VMEM((far, chips, per, rows, 2 * rows), BF16)
        near_w = pltpu.VMEM((near, blocks, rows, 2 * rows), BF16)
        result = pl.pallas_call(
            functools.partial(kernel, n, sub),
            out_shape=pltpu.VMEM(x.shape, BF16),
            in_specs=[pl.BlockSpec(memory_space=pl.ANY)] * 3,
            out_specs=pl.BlockSpec(memory_space=pltpu.VMEM),
            scratch_shapes=[
                buffer, buffer, buffer, buffer, temp, temp, far_w, far_w, near_w, near_w,
                pltpu.VMEM((2, far, chips, per // sub, rows, 2 * rows), BF16),
                pltpu.VMEM((2, chips, per, 2, rows, rows), BF16),
                dma((chunks,)), dma((chunks,)), dma((chunks,)), dma((chunks,)),
                dma((chunks,)), dma((chunks,)), dma((chunks,)), dma((chunks,)),
                dma((2, chunks)), dma((2, chunks)),
                dma((2,)), dma((2,)), dma((2, sub)), dma((2, sub)),
                dma((2,)),
            ],
            compiler_params=pltpu.CompilerParams(
                collective_id=0, has_side_effects=True, vmem_limit_bytes=56 * 2 ** 20),
        )(x, w_first.reshape(by_chip), w_second.reshape(by_chip))
        return result.reshape(signal.shape)

    row_spec = P(("dp", "sp"), None)
    weight_spec = P(None, "sp", None, None, None)
    return jax.shard_map(device_program, mesh=mesh, in_specs=(row_spec, weight_spec, weight_spec), out_specs=row_spec, check_vma=False)
```

```python
import functools
import math

import jax
import jax.numpy as jnp
from jax import lax
from jax.experimental import pallas as pl
from jax.experimental.pallas import tpu as pltpu
from jax.sharding import PartitionSpec as P

MESH = pl.DeviceIdType.MESH
BF16 = jnp.bfloat16
F32 = jnp.float32
CHUNK = 256
UNROLL = 8
CORES = 2


def gelu(x):
    return 0.5 * x * (1.0 + lax.erf(x * (0.5 ** 0.5)))


def mix_stage(src, dst, weights, step, act):
    pairs = src.shape[0] // 2
    unroll = min(UNROLL, pairs)

    @pl.loop(0, pairs // unroll)
    def _(it):
        for u in range(unroll):
            p = it * unroll + u
            i = (p // step) * (2 * step) + p % step
            j = i + step
            z = jnp.concatenate([src[i], src[j]], axis=0)
            w = jnp.concatenate([weights(i), weights(j)], axis=0)
            o = jnp.dot(w, z, preferred_element_type=F32).astype(BF16)
            if act:
                o = gelu(o.astype(F32)).astype(BF16)
            half = o.shape[0] // 2
            dst[i] = o[:half]
            dst[j] = o[half:]


def partner_stage(own, other, dst, weights):
    blocks = own.shape[0]
    unroll = min(UNROLL, blocks)

    @pl.loop(0, blocks // unroll)
    def _(it):
        for u in range(unroll):
            i = it * unroll + u
            z = jnp.concatenate([own[i], other[i]], axis=0)
            dst[i] = jnp.dot(weights(i), z, preferred_element_type=F32).astype(BF16)


def kernel(n, sub, x, wa, wb, out, r1, r2, r3, rp, tmp, tmq, ta, tb, la, lb, wz, raw,
           x_snd, x_rcv, o1_snd, o1_rcv, i2_snd, i2_rcv, o2_snd, o2_rcv, p_snd, p_rcv,
           z_snd, z_rcv, g_snd, g_rcv, raw_sem):
    me = lax.axis_index("sp")
    dp = lax.axis_index("dp")
    chip, core = me // CORES, me % CORES
    partner = {"sp": me + 1 - 2 * core}
    part = dp % sub
    base = dp - part
    chunks, blocks = r1.shape[0], r1.shape[1]
    stages = wa.shape[0]
    chips = n // CORES
    far = ta.shape[0]
    near = stages - far
    per = blocks // chips
    take = per // sub
    mine_l = pl.ds(part * take, take)

    def peer(t):
        if chips == 2:
            return (chip + 1) % chips
        pair, last = t // 2, t // (chips - 2)
        reach = chips // 2 - 1
        distance = (reach - pair) + core * (2 * pair + 1 - reach)
        offset = distance + (t % 2) * (chips - 2 * distance)
        return (chip + last * (chips // 2) + (1 - last) * offset) % chips

    def on(z):
        return {"sp": z * CORES + core}

    def group(k):
        return {"dp": base + (part + k) % sub}

    def cols(c):
        return pl.ds(pl.multiple_of(c * CHUNK, CHUNK), CHUNK)

    def of(z):
        return pl.ds(z * per, per)

    def wait_for(ref, sem):
        pltpu.make_async_copy(ref, ref, sem).wait()

    barrier = pltpu.get_barrier_semaphore()

    @pl.loop(0, chips - 1)
    def _(t):
        pl.semaphore_signal(barrier, inc=1, device_id=on(peer(t)), device_id_type=MESH)

    pl.semaphore_signal(barrier, inc=1, device_id=partner, device_id_type=MESH)
    for k in range(1, sub):
        pl.semaphore_signal(barrier, inc=1, device_id=group(k), device_id_type=MESH)
    pl.semaphore_wait(barrier, chips + sub - 1)

    jobs = [(m, s, True) for m in range(2) for s in range(far)]
    jobs += [(m, s, False) for m in range(2) for s in range(near)]
    w_of, t_of, l_of = (wa, wb), (ta, tb), (la, lb)

    def load(job):
        m, s, is_far = jobs[job]
        slot = job % 2
        if is_far:
            src = w_of[m].at[(0, near)[m] + s, :, mine_l]
            dst = raw.at[slot, :, pl.ds(0, take)]
        else:
            src, dst = w_of[m].at[(far, 0)[m] + s], raw.at[slot]
        return pltpu.make_async_copy(src, dst, raw_sem.at[slot])

    def prepare(job):
        m, s, is_far = jobs[job]
        slot = job % 2
        if is_far:
            upper = (chip // 2 ** (far - 1 - s, s)[m]) % 2 == 1

            @pl.loop(0, chips)
            def _(z):
                for b in range(take):
                    own, cross = raw[slot, z, b, 0], raw[slot, z, b, 1]
                    left, right = jnp.where(upper, cross, own), jnp.where(upper, own, cross)
                    wz[m, s, z, b] = jnp.concatenate([left, right], axis=-1)
        else:
            level = (near - 1 - s, s)[m]
            step = 2 ** level

            @pl.loop(0, blocks // 8)
            def _(it):
                for u in range(4):
                    p = it * 4 + u
                    i = (p // step) * (2 * step) + p % step
                    j = i + step
                    if level == near - 1:
                        i, j, swap = 2 * p, 2 * p + 1, False
                    else:
                        swap = True
                    first = [raw[slot, i // per, i % per, h] for h in range(2)]
                    second = [raw[slot, j // per, j % per, h] for h in range(2)]
                    l_of[m][s, i] = jnp.concatenate(first, axis=-1)
                    l_of[m][s, j] = jnp.concatenate(second[::-1] if swap else second, axis=-1)

    def run_jobs(first, last):
        for job in range(first, last):
            load(job).wait()
            prepare(job)
            if job + 2 < len(jobs):
                load(job + 2).start()

    def send_weights(m):
        @pl.loop(0, chips - 1)
        def _(t):
            z = peer(t)
            pltpu.make_async_remote_copy(
                src_ref=wz.at[m, :, z], dst_ref=t_of[m].at[:, chip, mine_l],
                send_sem=z_snd.at[m], recv_sem=z_rcv.at[m],
                device_id=on(z), device_id_type=MESH).start()

        for s in range(far):
            for b in range(take):
                t_of[m][s, chip, part * take + b] = wz[m, s, chip, b]

    def gather_copy(m, k):
        ref = t_of[m].at[:, :, mine_l]
        return pltpu.make_async_remote_copy(
            src_ref=ref, dst_ref=ref, send_sem=g_snd.at[m, k], recv_sem=g_rcv.at[m, k],
            device_id=group(k), device_id_type=MESH)

    def start_gather(m):
        wait_for(t_of[m].at[:, pl.ds(0, chips - 1), mine_l], z_rcv.at[m])
        for k in range(1, sub):
            gather_copy(m, k).start()

    def wait_gather(m):
        for k in range(1, sub):
            theirs = (part - k + sub) % sub
            wait_for(t_of[m].at[:, :, pl.ds(theirs * take, take)], g_rcv.at[m, k])

    def send_signal(c):
        @pl.loop(0, chips - 1)
        def _(t):
            z = peer(t)
            pltpu.make_async_remote_copy(
                src_ref=x.at[of(z), :, cols(c)], dst_ref=r1.at[c, of(chip)],
                send_sem=x_snd.at[c], recv_sem=x_rcv.at[c],
                device_id=on(z), device_id_type=MESH).start()

        pltpu.make_async_copy(x.at[of(chip), :, cols(c)], r1.at[c, of(chip)], x_rcv.at[c]).start()

    load(0).start()
    load(1).start()
    send_signal(0)
    run_jobs(0, far)
    send_weights(0)
    run_jobs(far, 2 * far)
    send_weights(1)

    @pl.loop(1, chunks)
    def _(c):
        send_signal(c)

    run_jobs(2 * far, len(jobs))
    start_gather(0)
    wait_gather(0)

    def far_weights(m, s):
        return lambda i: t_of[m][s, i // per, i % per]

    def near_weights(m, s):
        return lambda i: l_of[m][s, i]

    far_steps = [per * 2 ** s for s in range(far)]
    plan_t1 = [(far_weights(0, s), step, False) for s, step in enumerate(far_steps[::-1])]
    plan_t2 = [(far_weights(1, s), step, False) for s, step in enumerate(far_steps)]
    near_steps = [2 ** s for s in range(near - 1)]
    plan_n = [(near_weights(0, s + 1), step, step == 1) for s, step in enumerate(near_steps[::-1])]
    plan_n += [(near_weights(1, s), step, False) for s, step in enumerate(near_steps)]

    def run_far(buf, plan):
        src = buf
        for k, (weights, step, act) in enumerate(plan):
            dst = buf if k == len(plan) - 1 else (tmp, tmq)[k % 2]
            mix_stage(src, dst, weights, step, act)
            src = dst

    def others(ref, c):
        return ref.at[c, pl.ds(0, (chips - 1) * per)]

    def exchange(src, dst, c, snd, rcv):
        @pl.loop(0, chips - 1)
        def _(t):
            z = peer(t)
            pltpu.make_async_remote_copy(
                src_ref=src.at[c, of(z)], dst_ref=dst.at[c, of(chip)],
                send_sem=snd.at[c], recv_sem=rcv.at[c],
                device_id=on(z), device_id_type=MESH).start()

        dst[c, of(chip)] = src[c, of(chip)]

    @pl.loop(0, chunks)
    def _(c):
        wait_for(r1.at[c], x_rcv.at[c])
        run_far(r1.at[c], plan_t1)
        exchange(r1, r2, c, o1_snd, o1_rcv)

    start_gather(1)

    def partner_copy(k, src, dst, c):
        return pltpu.make_async_remote_copy(
            src_ref=src, dst_ref=dst, send_sem=p_snd.at[k, c], recv_sem=p_rcv.at[k, c],
            device_id=partner, device_id_type=MESH)

    @pl.loop(0, chunks)
    def _(c):
        wait_for(others(r2, c), o1_rcv.at[c])
        wait_for(others(r1, c), o1_snd.at[c])
        copy = partner_copy(0, r2.at[c], rp.at[c], c)
        copy.start()
        copy.wait_recv()
        partner_stage(r2.at[c], rp.at[c], tmp, near_weights(0, 0))
        copy.wait_send()
        src, dst = tmp, r2.at[c]
        for weights, step, act in plan_n:
            mix_stage(src, dst, weights, step, act)
            src, dst = dst, src
        copy = partner_copy(1, tmp, r1.at[c], c)
        copy.start()
        copy.wait_recv()
        partner_stage(tmp, r1.at[c], r2.at[c], near_weights(1, near - 1))
        copy.wait_send()
        exchange(r2, r3, c, i2_snd, i2_rcv)

    wait_gather(1)

    @pl.loop(0, chunks)
    def _(c):
        wait_for(others(r3, c), i2_rcv.at[c])
        run_far(r3.at[c], plan_t2)

        @pl.loop(0, chips - 1)
        def _(t):
            z = peer(t)
            pltpu.make_async_remote_copy(
                src_ref=r3.at[c, of(z)], dst_ref=out.at[of(chip), :, cols(c)],
                send_sem=o2_snd.at[c], recv_sem=o2_rcv.at[c],
                device_id=on(z), device_id_type=MESH).start()

        out[of(chip), :, cols(c)] = r3[c, of(chip)]

    for m in range(2):
        wait_for(t_of[m].at[:, pl.ds(0, chips - 1), mine_l], z_snd.at[m])
        for k in range(1, sub):
            gather_copy(m, k).wait_send()

    @pl.loop(0, chunks)
    def _(c):
        wait_for(others(r1, c), x_snd.at[c])
        wait_for(others(r2, c), i2_snd.at[c])
        wait_for(others(r3, c), o2_snd.at[c])
        wait_for(out.at[pl.ds(0, (chips - 1) * per), :, cols(c)], o2_rcv.at[c])


def solution(mesh):
    n = mesh.shape["sp"]
    groups = mesh.shape["dp"]
    chips = n // CORES
    far = int(math.log2(chips))

    def device_program(signal, w_first, w_second):
        stages, blocks, _, rows, _ = w_first.shape
        channels = signal.shape[1]
        chunks = channels // CHUNK
        near = stages - far
        per = blocks // chips
        sub = math.gcd(groups, per)
        x = signal.reshape(blocks, rows, channels)
        by_chip = (stages, chips, per, 2, rows, rows)
        dma = pltpu.SemaphoreType.DMA
        buffer = pltpu.VMEM((chunks, blocks, rows, CHUNK), BF16)
        temp = pltpu.VMEM((blocks, rows, CHUNK), BF16)
        far_w = pltpu.VMEM((far, chips, per, rows, 2 * rows), BF16)
        near_w = pltpu.VMEM((near, blocks, rows, 2 * rows), BF16)
        result = pl.pallas_call(
            functools.partial(kernel, n, sub),
            out_shape=pltpu.VMEM(x.shape, BF16),
            in_specs=[pl.BlockSpec(memory_space=pl.ANY)] * 3,
            out_specs=pl.BlockSpec(memory_space=pltpu.VMEM),
            scratch_shapes=[
                buffer, buffer, buffer, buffer, temp, temp, far_w, far_w, near_w, near_w,
                pltpu.VMEM((2, far, chips, per // sub, rows, 2 * rows), BF16),
                pltpu.VMEM((2, chips, per, 2, rows, rows), BF16),
                dma((chunks,)), dma((chunks,)), dma((chunks,)), dma((chunks,)),
                dma((chunks,)), dma((chunks,)), dma((chunks,)), dma((chunks,)),
                dma((2, chunks)), dma((2, chunks)),
                dma((2,)), dma((2,)), dma((2, sub)), dma((2, sub)),
                dma((2,)),
            ],
            compiler_params=pltpu.CompilerParams(
                collective_id=0, has_side_effects=True, vmem_limit_bytes=56 * 2 ** 20),
        )(x, w_first.reshape(by_chip), w_second.reshape(by_chip))
        return result.reshape(signal.shape)

    row_spec = P(("dp", "sp"), None)
    weight_spec = P(None, "sp", None, None, None)
    return jax.shard_map(device_program, mesh=mesh, in_specs=(row_spec, weight_spec, weight_spec), out_specs=row_spec, check_vma=False)
```
